32 devices in a mesh: seq: 16 (over z, x, core), grp: 2 (over y).
Axes of the slice: x: 2, y: 2, z: 4, core: 2. Of those that a mesh axis runs over, the one named last changes fastest.
Arguments:
- out_grad: bfloat16 [2, 3456, 1024], P('grp', 'seq'), may hold values from -6 to 6
- combine_logits: float32 [2, 3456, 64], P('grp', 'seq'), may hold values from -20 to 330
- expert_out: bfloat16 [2, 64, 1024], P('grp', 'seq'), may hold values from -6 to 6
- slot_in: bfloat16 [2, 64, 1024], P('grp', 'seq'), may hold values from -6 to 6
- router: bfloat16 [64, 1024], P('seq'), may hold values from -0.1875 to 0.1875
- w_gate: bfloat16 [64, 2048, 1024], P('seq', 'grp'), may hold values from -0.1875 to 0.1875
- w_up: bfloat16 [64, 2048, 1024], P('seq', 'grp'), may hold values from -0.1875 to 0.1875
- w_down: bfloat16 [64, 2048, 1024], P('seq', 'grp'), may hold values from -0.125 to 0.125
Outputs:
- token_grad: bfloat16 [2, 3456, 1024], P('grp', 'seq')
- slot_grad: float32 [2, 64, 1024], P('grp', 'seq')
- grad_gate: bfloat16 [64, 2048, 1024], P('seq', 'grp')
- grad_up: bfloat16 [64, 2048, 1024], P('seq', 'grp')
- grad_down: bfloat16 [64, 2048, 1024], P('seq', 'grp')
The draws below stay inside these ranges and needn't reach their ends.
All inputs are finite; a program needn't handle non-finite values.
Results may differ from the reference program's by a relative error of at most 0.028.
Values may be sent and summed in bfloat16 or wider, within the bound.
A program may use at most 128 MiB of HBM per device.

```python
import jax
import jax.numpy as jnp
from jax import lax

D = 1024
FF = 2048
EXPERTS = 64
TOKENS = 3456
SEQS = 2


def draw_combine_logits(key, part):
    keys = jax.random.split(key, 1)
    shape = (SEQS, TOKENS, EXPERTS)
    return jnp.clip(3.0 * jax.random.normal(keys[0], shape, jnp.float32), -18.0, 18.0)


def shard_levels(stream_key, shape, cuts, least, top_value):
    loudness = 1.0
    for dim, blocks in cuts:
        draws = jax.random.uniform(jax.random.fold_in(jax.random.fold_in(stream_key, 6), dim), (blocks,), jnp.float32, least / len(cuts), top_value / len(cuts))
        loudness = loudness * jnp.repeat(jnp.exp(draws), shape[dim] // blocks).reshape((-1,) + (1,) * (len(shape) - 1 - dim))
    return loudness


def centred(key, shape, spread, limit, cuts=(), kind=jnp.bfloat16):
    result = spread * jax.random.normal(key, shape, jnp.float32)
    if cuts:
        result = result * shard_levels(key, shape, cuts, -0.22, 0.18)
    return jnp.clip(result, -limit, limit).astype(kind)


def setup_inputs(seed: int = 0) -> dict:
    seeds = jax.random.split(jax.random.key(seed), 9)
    out_grad = centred(seeds[0], (SEQS, TOKENS, D), 1.0, 6.0, ((0, 2), (1, 16)))
    combine_logits = draw_combine_logits(jax.random.fold_in(seeds[8], 71), 0)
    expert_out = centred(seeds[2], (SEQS, EXPERTS, D), 1.0, 6.0, ((0, 2), (1, 16)))
    slot_in = centred(seeds[3], (SEQS, EXPERTS, D), 1.0, 6.0, ((0, 2), (1, 16)))
    router = centred(seeds[4], (EXPERTS, D), D ** -0.5, 0.1875, ((0, 16),))
    w_gate = centred(seeds[5], (EXPERTS, FF, D), D ** -0.5, 0.1875, ((0, 16), (1, 2)))
    w_up = centred(seeds[6], (EXPERTS, FF, D), D ** -0.5, 0.1875, ((0, 16), (1, 2)))
    w_down = centred(seeds[7], (EXPERTS, FF, D), FF ** -0.5, 0.125, ((0, 16), (1, 2)))
    return dict(out_grad=out_grad, combine_logits=combine_logits, expert_out=expert_out, slot_in=slot_in, router=router, w_gate=w_gate, w_up=w_up, w_down=w_down)


def sequence_part(items, router):
    grads, logits, outputs = items
    probs = jax.nn.softmax(logits, axis=-1)
    probs_bf = probs.astype(jnp.bfloat16)
    slot_out = lax.dot_general(probs_bf, grads, (((0,), (0,)), ((), ())), preferred_element_type=jnp.float32)
    weight_grad = lax.dot_general(grads, outputs, (((1,), (1,)), ((), ())), preferred_element_type=jnp.float32)
    centre = jnp.sum(weight_grad * probs, axis=-1, keepdims=True)
    logit_grad = (probs * (weight_grad - centre)).astype(jnp.bfloat16)
    token_grad = jnp.dot(logit_grad, router, preferred_element_type=jnp.float32).astype(jnp.bfloat16)
    return token_grad, slot_out.astype(jnp.bfloat16)


def expert_part(items):
    inputs, out_grads, w_gate, w_up, w_down = items
    dims = (((1,), (1,)), ((), ()))
    gate = lax.dot_general(inputs, w_gate, dims, preferred_element_type=jnp.float32)
    upper = lax.dot_general(inputs, w_up, dims, preferred_element_type=jnp.float32)
    sig = jax.nn.sigmoid(gate)
    hidden = (gate * sig * upper).astype(jnp.bfloat16)
    hidden_grad = lax.dot_general(out_grads, w_down, dims, preferred_element_type=jnp.float32)
    up_grad = (hidden_grad * gate * sig).astype(jnp.bfloat16)
    gate_grad = (hidden_grad * upper * sig * (1.0 + gate * (1.0 - sig))).astype(jnp.bfloat16)
    slot_grad = jnp.dot(gate_grad, w_gate, preferred_element_type=jnp.float32) + jnp.dot(up_grad, w_up, preferred_element_type=jnp.float32)
    outer = (((0,), (0,)), ((), ()))
    grad_gate = lax.dot_general(gate_grad, inputs, outer, preferred_element_type=jnp.float32).astype(jnp.bfloat16)
    grad_up = lax.dot_general(up_grad, inputs, outer, preferred_element_type=jnp.float32).astype(jnp.bfloat16)
    grad_down = lax.dot_general(hidden, out_grads, outer, preferred_element_type=jnp.float32).astype(jnp.bfloat16)
    return slot_grad, grad_gate, grad_up, grad_down


def reference(out_grad, combine_logits, expert_out, slot_in, router, w_gate, w_up, w_down):
    token_grad, slot_out_bf = lax.map(lambda items: sequence_part(items, router), (out_grad, combine_logits, expert_out))
    per_expert = (jnp.transpose(slot_in, (1, 0, 2)), jnp.transpose(slot_out_bf, (1, 0, 2)), w_gate, w_up, w_down)
    slot_grad, grad_gate, grad_up, grad_down = lax.map(expert_part, per_expert)
    return token_grad, jnp.transpose(slot_grad, (1, 0, 2)), grad_gate, grad_up, grad_down
```

```python
import functools

import jax
import jax.numpy as jnp
from jax import lax
from jax.experimental import pallas as pl
from jax.experimental.pallas import tpu as pltpu
from jax.sharding import PartitionSpec as P

MESH = pl.DeviceIdType.MESH
F32 = jnp.float32
BF16 = jnp.bfloat16
NT = (((1,), (1,)), ((), ()))
TN = (((0,), (0,)), ((), ()))


def rows_of(ref, count):
    return jnp.concatenate([ref[i].astype(F32) for i in range(count)], axis=0).astype(BF16)


def exchange_kernel(
    nseq, ngrp,
    grad_hbm, logit_hbm, eout_hbm, slot_hbm, router_hbm, gate_hbm, up_hbm, down_hbm,
    acts_ref, pair_ref, lgrad_ref, rout_ref, sgrad_ref,
    grad, logit, gate_w, up_w, down_w, part_out, part_in, pieces, slots, outs, back_out, back_in,
    load_sem, w_sem, part_ssem, part_rsem, piece_ssem, piece_rsem,
    slot_ssem, slot_rsem, out_ssem, out_rsem, back_ssem, back_rsem,
):
    s_me = lax.axis_index("seq")
    g_me = lax.axis_index("grp")
    experts = slots.shape[1]

    barrier = pltpu.get_barrier_semaphore()

    def greet_seq(d, c):
        pl.semaphore_signal(barrier, inc=1, device_id={"seq": lax.rem(s_me + d, nseq)}, device_id_type=MESH)
        return c

    def greet_grp(d, c):
        pl.semaphore_signal(barrier, inc=1, device_id={"grp": lax.rem(g_me + d, ngrp)}, device_id_type=MESH)
        return c

    lax.fori_loop(1, ngrp, greet_grp, 0)
    lax.fori_loop(1, nseq, greet_seq, 0)

    loads = [
        pltpu.make_async_copy(logit_hbm.at[0], logit, load_sem.at[0]),
        pltpu.make_async_copy(grad_hbm.at[0], grad, load_sem.at[1]),
        pltpu.make_async_copy(slot_hbm.at[0], slots.at[g_me], load_sem.at[2]),
        pltpu.make_async_copy(eout_hbm.at[0], pieces.at[s_me, 0], load_sem.at[3]),
        pltpu.make_async_copy(router_hbm, pieces.at[s_me, 1], load_sem.at[4]),
    ]
    for c in loads:
        c.start()
    w_loads = {}
    for m, (src, dst) in enumerate(((gate_hbm, gate_w), (up_hbm, up_w), (down_hbm, down_w))):
        for e in range(experts):
            w_loads[m, e] = pltpu.make_async_copy(src.at[e], dst.at[e], w_sem.at[m, e])
    for e in range(experts):
        w_loads[0, e].start()
        w_loads[1, e].start()
    for e in range(experts):
        w_loads[2, e].start()

    def part_copy(d):
        to = lax.rem(s_me + d, nseq)
        return pltpu.make_async_remote_copy(
            src_ref=part_out.at[to], dst_ref=part_in.at[s_me],
            send_sem=part_ssem.at[to], recv_sem=part_rsem.at[s_me],
            device_id={"seq": to}, device_id_type=MESH)

    def piece_copy(d):
        to = lax.rem(s_me + d, nseq)
        return pltpu.make_async_remote_copy(
            src_ref=pieces.at[s_me], dst_ref=pieces.at[s_me],
            send_sem=piece_ssem.at[to], recv_sem=piece_rsem.at[s_me],
            device_id={"seq": to}, device_id_type=MESH)

    def grp_copy(d, src, dst, ssem, rsem):
        to = lax.rem(g_me + d, ngrp)
        return pltpu.make_async_remote_copy(
            src_ref=src.at[to] if src is not dst else src.at[g_me], dst_ref=dst.at[g_me],
            send_sem=ssem.at[to], recv_sem=rsem.at[g_me],
            device_id={"grp": to}, device_id_type=MESH)

    def seq_arrived(d, buf, rsem, ssem):
        at = lax.rem(s_me + d, nseq)
        pltpu.make_async_remote_copy(
            src_ref=buf.at[at], dst_ref=buf.at[at], send_sem=ssem.at[at], recv_sem=rsem.at[at],
            device_id={"seq": at}, device_id_type=MESH).wait_recv()

    def grp_arrived(d, buf, rsem, ssem):
        at = lax.rem(g_me + d, ngrp)
        pltpu.make_async_remote_copy(
            src_ref=buf.at[at], dst_ref=buf.at[at], send_sem=ssem.at[at], recv_sem=rsem.at[at],
            device_id={"grp": at}, device_id_type=MESH).wait_recv()

    def each(low, high, fn):
        def step(d, c):
            fn(d)
            return c
        lax.fori_loop(low, high, step, 0)

    loads[0].wait()
    z = logit[...]
    z = jnp.exp(z - jnp.max(z, axis=-1, keepdims=True))
    probs = z / jnp.sum(z, axis=-1, keepdims=True)
    logit[...] = probs
    loads[1].wait()
    share = lax.dot_general(probs.astype(BF16), grad[...], TN, preferred_element_type=F32)
    for j in range(nseq):
        part_out[j] = share[j * experts:(j + 1) * experts].astype(BF16)
    part_in[s_me] = part_out[s_me]
    for c in loads[2:]:
        c.wait()

    pl.semaphore_wait(barrier, (nseq - 1) + (ngrp - 1))
    each(1, ngrp, lambda d: grp_copy(d, slots, slots, slot_ssem, slot_rsem).start())
    each(1, nseq, lambda d: part_copy(d).start())
    each(1, nseq, lambda d: piece_copy(d).start())

    rows = ngrp * experts
    width = gate_w.shape[1]
    own = lax.rem(lax.broadcasted_iota(jnp.int32, (rows, width), 0), experts)

    each(1, ngrp, lambda d: grp_arrived(d, slots, slot_rsem, slot_ssem))
    x = rows_of(slots, ngrp)
    pair_ref[0] = x

    gate = jnp.zeros((rows, width), F32)
    upper = jnp.zeros((rows, width), F32)

    def project(e, gate, upper):
        w_loads[0, e].wait()
        gate = jnp.where(own == e, lax.dot_general(x, gate_w[e], NT, preferred_element_type=F32), gate)
        w_loads[1, e].wait()
        upper = jnp.where(own == e, lax.dot_general(x, up_w[e], NT, preferred_element_type=F32), upper)
        return gate, upper

    early = experts // 2
    for e in range(early):
        gate, upper = project(e, gate, upper)

    each(1, nseq, lambda d: seq_arrived(d, part_in, part_rsem, part_ssem))
    outs[g_me] = jnp.sum(part_in[...].astype(F32), axis=0).astype(BF16)
    each(1, ngrp, lambda d: grp_copy(d, outs, outs, out_ssem, out_rsem).start())

    for e in range(early, experts):
        gate, upper = project(e, gate, upper)
    sig = jax.nn.sigmoid(gate)
    act = gate * sig
    acts_ref[2] = (act * upper).astype(BF16)

    each(1, ngrp, lambda d: grp_arrived(d, outs, out_rsem, out_ssem))
    so = rows_of(outs, ngrp)
    pair_ref[1] = so
    hgrad = jnp.zeros((rows, width), F32)
    for e in range(experts):
        w_loads[2, e].wait()
        hgrad = jnp.where(own == e, lax.dot_general(so, down_w[e], NT, preferred_element_type=F32), hgrad)
    up_grad = (hgrad * gate * sig).astype(BF16)
    gate_grad = (hgrad * upper * sig * (1.0 + gate * (1.0 - sig))).astype(BF16)
    acts_ref[0] = gate_grad
    acts_ref[1] = up_grad

    gate_f, up_f = gate_grad.astype(F32), up_grad.astype(F32)
    total = jnp.zeros((rows, x.shape[1]), F32)
    for e in range(experts):
        total += jnp.dot(jnp.where(own == e, gate_f, 0.0).astype(BF16), gate_w[e], preferred_element_type=F32)
        total += jnp.dot(jnp.where(own == e, up_f, 0.0).astype(BF16), up_w[e], preferred_element_type=F32)
    for g in range(ngrp):
        back_out[g] = total[g * experts:(g + 1) * experts].astype(BF16)
    back_in[g_me] = back_out[g_me]
    each(1, ngrp, lambda d: grp_copy(d, back_out, back_in, back_ssem, back_rsem).start())

    each(1, nseq, lambda d: seq_arrived(d, pieces, piece_rsem, piece_ssem))
    eout = rows_of(pieces.at[:, 0], nseq)
    rout_ref[...] = rows_of(pieces.at[:, 1], nseq)
    wgrad = lax.dot_general(grad[...], eout, NT, preferred_element_type=F32)
    p = logit[...]
    centre = jnp.sum(wgrad * p, axis=-1, keepdims=True)
    lgrad_ref[...] = (p * (wgrad - centre)).astype(BF16)

    each(1, ngrp, lambda d: grp_arrived(d, back_in, back_rsem, back_ssem))
    sgrad_ref[...] = jnp.sum(back_in[...].astype(F32), axis=0)

    each(1, nseq, lambda d: part_copy(d).wait_send())
    each(1, nseq, lambda d: piece_copy(d).wait_send())
    each(1, ngrp, lambda d: grp_copy(d, slots, slots, slot_ssem, slot_rsem).wait_send())
    each(1, ngrp, lambda d: grp_copy(d, outs, outs, out_ssem, out_rsem).wait_send())
    each(1, ngrp, lambda d: grp_copy(d, back_out, back_in, back_ssem, back_rsem).wait_send())


def write_kernel(experts, acts_ref, pair_ref, lgrad_ref, rout_ref, sgrad_in, tgrad_ref, sgrad_ref, gg_ref, gu_ref, gd_ref):
    e = pl.program_id(0)

    @pl.when((e == 0) & (pl.program_id(1) == 0))
    def _():
        tgrad_ref[0] = jnp.dot(lgrad_ref[...], rout_ref[...], preferred_element_type=F32).astype(BF16)
        sgrad_ref[0] = sgrad_in[...]

    shape = acts_ref.shape[1:]
    own = lax.rem(lax.broadcasted_iota(jnp.int32, shape, 0), experts) == e
    for k, (src, out) in enumerate(((0, gg_ref), (0, gu_ref), (1, gd_ref))):
        a = jnp.where(own, acts_ref[k].astype(F32), 0.0).astype(BF16)
        out[0] = lax.dot_general(a, pair_ref[src], TN, preferred_element_type=F32).astype(BF16)


def per_device(nseq, ngrp, out_grad, combine_logits, expert_out, slot_in, router, w_gate, w_up, w_down):
    _, tokens, dim = out_grad.shape
    total_experts = combine_logits.shape[2]
    experts, width, _ = w_gate.shape
    rows = ngrp * experts
    DMA = pltpu.SemaphoreType.DMA
    anyspec = pl.BlockSpec(memory_space=pl.ANY)
    vspec = pl.BlockSpec(memory_space=pltpu.VMEM)
    acts, pair, lgrad, rout, sgrad = pl.pallas_call(
        functools.partial(exchange_kernel, nseq, ngrp),
        out_shape=(
            jax.ShapeDtypeStruct((3, rows, width), BF16),
            jax.ShapeDtypeStruct((2, rows, dim), BF16),
            jax.ShapeDtypeStruct((tokens, total_experts), BF16),
            jax.ShapeDtypeStruct((total_experts, dim), BF16),
            jax.ShapeDtypeStruct((experts, dim), F32),
        ),
        in_specs=[anyspec] * 8,
        out_specs=(vspec,) * 5,
        scratch_shapes=[
            pltpu.VMEM((tokens, dim), BF16),
            pltpu.VMEM((tokens, total_experts), F32),
            pltpu.VMEM((experts, width, dim), BF16),
            pltpu.VMEM((experts, width, dim), BF16),
            pltpu.VMEM((experts, width, dim), BF16),
            pltpu.VMEM((nseq, experts, dim), BF16),
            pltpu.VMEM((nseq, experts, dim), BF16),
            pltpu.VMEM((nseq, 2, experts, dim), BF16),
            pltpu.VMEM((ngrp, experts, dim), BF16),
            pltpu.VMEM((ngrp, experts, dim), BF16),
            pltpu.VMEM((ngrp, experts, dim), BF16),
            pltpu.VMEM((ngrp, experts, dim), BF16),
            DMA((5,)), DMA((3, experts)),
            DMA((nseq,)), DMA((nseq,)), DMA((nseq,)), DMA((nseq,)),
            DMA((ngrp,)), DMA((ngrp,)), DMA((ngrp,)), DMA((ngrp,)), DMA((ngrp,)), DMA((ngrp,)),
        ],
        compiler_params=pltpu.CompilerParams(
            collective_id=0, has_side_effects=True, vmem_limit_bytes=48 * 1024 * 1024),
        name="exchange",
    )(out_grad, combine_logits, expert_out, slot_in, router, w_gate, w_up, w_down)

    cut = 256 if width % 256 == 0 else width
    whole = lambda *shape: pl.BlockSpec(shape, lambda e, j: (0,) * len(shape))
    big = pl.BlockSpec((1, cut, dim), lambda e, j: (e, j, 0))
    return pl.pallas_call(
        functools.partial(write_kernel, experts),
        grid=(experts, width // cut),
        out_shape=(
            jax.ShapeDtypeStruct((1, tokens, dim), BF16),
            jax.ShapeDtypeStruct((1, experts, dim), F32),
        ) + (jax.ShapeDtypeStruct((experts, width, dim), BF16),) * 3,
        in_specs=[
            pl.BlockSpec((3, rows, cut), lambda e, j: (0, 0, j)),
            whole(2, rows, dim), whole(tokens, total_experts), whole(total_experts, dim), whole(experts, dim),
        ],
        out_specs=(whole(1, tokens, dim), whole(1, experts, dim), big, big, big),
        compiler_params=pltpu.CompilerParams(vmem_limit_bytes=24 * 1024 * 1024),
        name="write",
    )(acts, pair, lgrad, rout, sgrad)


def solution(mesh):
    return jax.shard_map(
        functools.partial(per_device, mesh.shape["seq"], mesh.shape["grp"]),
        mesh=mesh,
        in_specs=(
            P("grp", "seq", None),
            P("grp", "seq", None),
            P("grp", "seq", None),
            P("grp", "seq", None),
            P("seq", None),
            P("seq", "grp", None),
            P("seq", "grp", None),
            P("seq", "grp", None),
        ),
        out_specs=(
            P("grp", "seq", None),
            P("grp", "seq", None),
            P("seq", "grp", None),
            P("seq", "grp", None),
            P("seq", "grp", None),
        ),
        check_vma=False,
    )
```

```python
import functools

import jax
import jax.numpy as jnp
from jax import lax
from jax.experimental import pallas as pl
from jax.experimental.pallas import tpu as pltpu
from jax.sharding import PartitionSpec as P

MESH = pl.DeviceIdType.MESH
F32 = jnp.float32
BF16 = jnp.bfloat16
NT = (((1,), (1,)), ((), ()))
TN = (((0,), (0,)), ((), ()))


def rows_of(ref, count):
    return jnp.concatenate([ref[i].astype(F32) for i in range(count)], axis=0).astype(BF16)


def exchange_kernel(
    nseq, ngrp,
    grad_hbm, logit_hbm, eout_hbm, slot_hbm, router_hbm, gate_hbm, up_hbm, down_hbm,
    acts_ref, pair_ref, lgrad_ref, rout_ref, sgrad_ref,
    grad, logit, gate_w, up_w, down_w, part_out, part_in, pieces, slots, outs, back_out, back_in,
    load_sem, w_sem, part_ssem, part_rsem, piece_ssem, piece_rsem,
    slot_ssem, slot_rsem, out_ssem, out_rsem, back_ssem, back_rsem,
):
    s_me = lax.axis_index("seq")
    g_me = lax.axis_index("grp")
    experts = slots.shape[1]

    barrier = pltpu.get_barrier_semaphore()

    def greet_seq(d, c):
        pl.semaphore_signal(barrier, inc=1, device_id={"seq": lax.rem(s_me + d, nseq)}, device_id_type=MESH)
        return c

    def greet_grp(d, c):
        pl.semaphore_signal(barrier, inc=1, device_id={"grp": lax.rem(g_me + d, ngrp)}, device_id_type=MESH)
        return c

    lax.fori_loop(1, ngrp, greet_grp, 0)
    lax.fori_loop(1, nseq, greet_seq, 0)

    loads = [
        pltpu.make_async_copy(logit_hbm, logit, load_sem.at[0]),
        pltpu.make_async_copy(grad_hbm.at[0], grad, load_sem.at[1]),
        pltpu.make_async_copy(slot_hbm.at[0], slots.at[g_me], load_sem.at[2]),
        pltpu.make_async_copy(eout_hbm.at[0], pieces.at[s_me, 0], load_sem.at[3]),
        pltpu.make_async_copy(router_hbm, pieces.at[s_me, 1], load_sem.at[4]),
    ]
    for c in loads:
        c.start()
    w_loads = {}
    for m, (src, dst) in enumerate(((gate_hbm, gate_w), (up_hbm, up_w), (down_hbm, down_w))):
        for e in range(experts):
            w_loads[m, e] = pltpu.make_async_copy(src.at[e], dst.at[e], w_sem.at[m, e])
    for e in range(experts):
        w_loads[0, e].start()
        w_loads[1, e].start()
    for e in range(experts):
        w_loads[2, e].start()

    def part_copy(d):
        to = lax.rem(s_me + d, nseq)
        return pltpu.make_async_remote_copy(
            src_ref=part_out.at[to], dst_ref=part_in.at[s_me],
            send_sem=part_ssem.at[to], recv_sem=part_rsem.at[s_me],
            device_id={"seq": to}, device_id_type=MESH)

    def piece_copy(d):
        to = lax.rem(s_me + d, nseq)
        return pltpu.make_async_remote_copy(
            src_ref=pieces.at[s_me], dst_ref=pieces.at[s_me],
            send_sem=piece_ssem.at[to], recv_sem=piece_rsem.at[s_me],
            device_id={"seq": to}, device_id_type=MESH)

    def grp_copy(d, src, dst, ssem, rsem):
        to = lax.rem(g_me + d, ngrp)
        return pltpu.make_async_remote_copy(
            src_ref=src.at[to] if src is not dst else src.at[g_me], dst_ref=dst.at[g_me],
            send_sem=ssem.at[to], recv_sem=rsem.at[g_me],
            device_id={"grp": to}, device_id_type=MESH)

    def seq_arrived(d, buf, rsem, ssem):
        at = lax.rem(s_me + d, nseq)
        pltpu.make_async_remote_copy(
            src_ref=buf.at[at], dst_ref=buf.at[at], send_sem=ssem.at[at], recv_sem=rsem.at[at],
            device_id={"seq": at}, device_id_type=MESH).wait_recv()

    def grp_arrived(d, buf, rsem, ssem):
        at = lax.rem(g_me + d, ngrp)
        pltpu.make_async_remote_copy(
            src_ref=buf.at[at], dst_ref=buf.at[at], send_sem=ssem.at[at], recv_sem=rsem.at[at],
            device_id={"grp": at}, device_id_type=MESH).wait_recv()

    def each(low, high, fn):
        def step(d, c):
            fn(d)
            return c
        lax.fori_loop(low, high, step, 0)

    loads[0].wait()
    z = logit[...]
    z = jnp.exp(z - jnp.max(z, axis=0, keepdims=True))
    probs = z / jnp.sum(z, axis=0, keepdims=True)
    logit[...] = probs
    loads[1].wait()
    share = jnp.dot(probs.astype(BF16), grad[...], preferred_element_type=F32)
    for j in range(nseq):
        part_out[j] = share[j * experts:(j + 1) * experts].astype(BF16)
    part_in[s_me] = part_out[s_me]
    for c in loads[2:]:
        c.wait()

    pl.semaphore_wait(barrier, (nseq - 1) + (ngrp - 1))
    each(1, ngrp, lambda d: grp_copy(d, slots, slots, slot_ssem, slot_rsem).start())
    each(1, nseq, lambda d: part_copy(d).start())
    each(1, nseq, lambda d: piece_copy(d).start())

    rows = ngrp * experts
    width = gate_w.shape[1]
    own = lax.rem(lax.broadcasted_iota(jnp.int32, (rows, width), 0), experts)

    each(1, ngrp, lambda d: grp_arrived(d, slots, slot_rsem, slot_ssem))
    x = rows_of(slots, ngrp)
    pair_ref[0] = x

    gate = jnp.zeros((rows, width), F32)
    upper = jnp.zeros((rows, width), F32)

    def project(e, gate, upper):
        w_loads[0, e].wait()
        gate = jnp.where(own == e, lax.dot_general(x, gate_w[e], NT, preferred_element_type=F32), gate)
        w_loads[1, e].wait()
        upper = jnp.where(own == e, lax.dot_general(x, up_w[e], NT, preferred_element_type=F32), upper)
        return gate, upper

    early = experts // 2
    for e in range(early):
        gate, upper = project(e, gate, upper)

    each(1, nseq, lambda d: seq_arrived(d, part_in, part_rsem, part_ssem))
    outs[g_me] = jnp.sum(part_in[...].astype(F32), axis=0).astype(BF16)
    each(1, ngrp, lambda d: grp_copy(d, outs, outs, out_ssem, out_rsem).start())

    for e in range(early, experts):
        gate, upper = project(e, gate, upper)
    sig = jax.nn.sigmoid(gate)
    act = gate * sig
    acts_ref[2] = (act * upper).astype(BF16)

    each(1, ngrp, lambda d: grp_arrived(d, outs, out_rsem, out_ssem))
    so = rows_of(outs, ngrp)
    pair_ref[1] = so
    hgrad = jnp.zeros((rows, width), F32)
    for e in range(experts):
        w_loads[2, e].wait()
        hgrad = jnp.where(own == e, lax.dot_general(so, down_w[e], NT, preferred_element_type=F32), hgrad)
    up_grad = (hgrad * gate * sig).astype(BF16)
    gate_grad = (hgrad * upper * sig * (1.0 + gate * (1.0 - sig))).astype(BF16)
    acts_ref[0] = gate_grad
    acts_ref[1] = up_grad

    gate_f, up_f = gate_grad.astype(F32), up_grad.astype(F32)
    total = jnp.zeros((rows, x.shape[1]), F32)
    for e in range(experts):
        total += jnp.dot(jnp.where(own == e, gate_f, 0.0).astype(BF16), gate_w[e], preferred_element_type=F32)
        total += jnp.dot(jnp.where(own == e, up_f, 0.0).astype(BF16), up_w[e], preferred_element_type=F32)
    for g in range(ngrp):
        back_out[g] = total[g * experts:(g + 1) * experts].astype(BF16)
    back_in[g_me] = back_out[g_me]
    each(1, ngrp, lambda d: grp_copy(d, back_out, back_in, back_ssem, back_rsem).start())

    each(1, nseq, lambda d: seq_arrived(d, pieces, piece_rsem, piece_ssem))
    eout = rows_of(pieces.at[:, 0], nseq)
    rout_ref[...] = rows_of(pieces.at[:, 1], nseq)
    wgrad = lax.dot_general(eout, grad[...], NT, preferred_element_type=F32)
    p = logit[...]
    centre = jnp.sum(wgrad * p, axis=0, keepdims=True)
    lgrad_ref[...] = (p * (wgrad - centre)).astype(BF16)

    each(1, ngrp, lambda d: grp_arrived(d, back_in, back_rsem, back_ssem))
    sgrad_ref[...] = jnp.sum(back_in[...].astype(F32), axis=0)

    each(1, nseq, lambda d: part_copy(d).wait_send())
    each(1, nseq, lambda d: piece_copy(d).wait_send())
    each(1, ngrp, lambda d: grp_copy(d, slots, slots, slot_ssem, slot_rsem).wait_send())
    each(1, ngrp, lambda d: grp_copy(d, outs, outs, out_ssem, out_rsem).wait_send())
    each(1, ngrp, lambda d: grp_copy(d, back_out, back_in, back_ssem, back_rsem).wait_send())


def write_kernel(
    experts, cut,
    acts_ref, pair_ref, lgrad_ref, rout_ref, sgrad_in,
    tgrad_hbm, sgrad_hbm, gg_hbm, gu_hbm, gd_hbm,
    staged, tokens, sem, small_sem,
):
    outs = (gg_hbm, gu_hbm, gd_hbm)
    width = acts_ref.shape[2]
    own = lax.rem(lax.broadcasted_iota(jnp.int32, acts_ref.shape[1:], 0), experts)

    def chunk(k, e, j):
        at = pl.ds(j * cut, cut)
        return pltpu.make_async_copy(staged.at[k, e, at], outs[k].at[e, at], sem.at[k, e, j])

    def expert(e, c):
        for k, src in enumerate((0, 0, 1)):
            a = jnp.where(own == e, acts_ref[k].astype(F32), 0.0).astype(BF16)
            for j in range(width // cut):
                at = slice(j * cut, (j + 1) * cut)
                staged[k, e, at] = lax.dot_general(
                    a[:, at], pair_ref[src], TN, preferred_element_type=F32).astype(BF16)
                chunk(k, e, j).start()
        return c

    lax.fori_loop(0, experts, expert, 0)
    tokens[...] = lax.dot_general(lgrad_ref[...], rout_ref[...], TN, preferred_element_type=F32).astype(BF16)
    small = [
        pltpu.make_async_copy(tokens, tgrad_hbm.at[0], small_sem.at[0]),
        pltpu.make_async_copy(sgrad_in, sgrad_hbm.at[0], small_sem.at[1]),
    ]
    for c in small:
        c.start()
    for e in range(experts):
        for k in range(3):
            for j in range(width // cut):
                chunk(k, e, j).wait()
    for c in small:
        c.wait()


def per_device(nseq, ngrp, out_grad, combine_logits, expert_out, slot_in, router, w_gate, w_up, w_down):
    _, tokens, dim = out_grad.shape
    total_experts = combine_logits.shape[2]
    experts, width, _ = w_gate.shape
    rows = ngrp * experts
    DMA = pltpu.SemaphoreType.DMA
    anyspec = pl.BlockSpec(memory_space=pltpu.HBM)
    vspec = pl.BlockSpec(memory_space=pltpu.VMEM)
    acts, pair, lgrad, rout, sgrad = pl.pallas_call(
        functools.partial(exchange_kernel, nseq, ngrp),
        out_shape=(
            jax.ShapeDtypeStruct((3, rows, width), BF16),
            jax.ShapeDtypeStruct((2, rows, dim), BF16),
            jax.ShapeDtypeStruct((total_experts, tokens), BF16),
            jax.ShapeDtypeStruct((total_experts, dim), BF16),
            jax.ShapeDtypeStruct((experts, dim), F32),
        ),
        in_specs=[anyspec] * 8,
        out_specs=(vspec,) * 5,
        scratch_shapes=[
            pltpu.VMEM((tokens, dim), BF16),
            pltpu.VMEM((total_experts, tokens), F32),
            pltpu.VMEM((experts, width, dim), BF16),
            pltpu.VMEM((experts, width, dim), BF16),
            pltpu.VMEM((experts, width, dim), BF16),
            pltpu.VMEM((nseq, experts, dim), BF16),
            pltpu.VMEM((nseq, experts, dim), BF16),
            pltpu.VMEM((nseq, 2, experts, dim), BF16),
            pltpu.VMEM((ngrp, experts, dim), BF16),
            pltpu.VMEM((ngrp, experts, dim), BF16),
            pltpu.VMEM((ngrp, experts, dim), BF16),
            pltpu.VMEM((ngrp, experts, dim), BF16),
            DMA((5,)), DMA((3, experts)),
            DMA((nseq,)), DMA((nseq,)), DMA((nseq,)), DMA((nseq,)),
            DMA((ngrp,)), DMA((ngrp,)), DMA((ngrp,)), DMA((ngrp,)), DMA((ngrp,)), DMA((ngrp,)),
        ],
        compiler_params=pltpu.CompilerParams(
            collective_id=0, has_side_effects=True, vmem_limit_bytes=48 * 1024 * 1024),
        name="exchange",
    )(*(pltpu.with_memory_space_constraint(a, pltpu.HBM) for a in (
        out_grad, jnp.transpose(combine_logits[0]), expert_out, slot_in, router, w_gate, w_up, w_down)))

    cut = 256 if width % 256 == 0 else width
    return pl.pallas_call(
        functools.partial(write_kernel, experts, cut),
        out_shape=(
            jax.ShapeDtypeStruct((1, tokens, dim), BF16),
            jax.ShapeDtypeStruct((1, experts, dim), F32),
        ) + (jax.ShapeDtypeStruct((experts, width, dim), BF16),) * 3,
        in_specs=[vspec] * 5,
        out_specs=(pl.BlockSpec(memory_space=pltpu.HBM),) * 5,
        scratch_shapes=[
            pltpu.VMEM((3, experts, width, dim), BF16),
            pltpu.VMEM((tokens, dim), BF16),
            DMA((3, experts, width // cut)),
            DMA((2,)),
        ],
        compiler_params=pltpu.CompilerParams(vmem_limit_bytes=40 * 1024 * 1024),
        name="write",
    )(acts, pair, lgrad, rout, sgrad)


def solution(mesh):
    return jax.shard_map(
        functools.partial(per_device, mesh.shape["seq"], mesh.shape["grp"]),
        mesh=mesh,
        in_specs=(
            P("grp", "seq", None),
            P("grp", "seq", None),
            P("grp", "seq", None),
            P("grp", "seq", None),
            P("seq", None),
            P("seq", "grp", None),
            P("seq", "grp", None),
            P("seq", "grp", None),
        ),
        out_specs=(
            P("grp", "seq", None),
            P("grp", "seq", None),
            P("seq", "grp", None),
            P("seq", "grp", None),
            P("seq", "grp", None),
        ),
        check_vma=False,
    )
```
